32 devices in a mesh: dp: 4 (over y, x), expert: 8 (over z, core).
Axes of the slice: x: 2, y: 2, z: 4, core: 2. Of those that a mesh axis runs over, the one named last changes fastest.
Arguments:
- tokens: bfloat16 [16384, 2048], P(('dp', 'expert')), may hold values from -6 to 6
- expert_ids: int32 [16384, 1], P(('dp', 'expert')), may hold values from 0 to 7; in each aligned block of 512 rows (0 to 511, 512 to 1023, ...) at most 128 rows name the same one
- gate_proj: bfloat16 [8, 2048, 768], P('expert'), may hold values from -0.125 to 0.125
- up_proj: bfloat16 [8, 2048, 768], P('expert'), may hold values from -0.125 to 0.125
- down_proj: bfloat16 [8, 768, 2048], P('expert'), may hold values from -0.21875 to 0.21875
Outputs:
- mixed: bfloat16 [16384, 2048], P(('dp', 'expert'))
- slot_index: int32 [16384], P(('dp', 'expert'))
The draws below stay inside these ranges and needn't reach their ends.
Inputs may be any that keep to these rules, and one draw needn't show every extreme that they name: `expert_ids`: among the rows of one device no expert is named more than 128 times; in some devices' rows one expert is named exactly 128 times.
All inputs are finite; a program needn't handle non-finite values.
Results may differ from the reference program's by a relative error of at most 0.0046.
The reference program's roundings to bfloat16 on the way (of `hidden`) count: a program that leaves them out, or rounds other values in their place, can miss the bound.
Values may be sent and summed in bfloat16 or wider, within the bound.
No kernel may reach another device: no remote copies, remote signals or barrier semaphores. Data moves between devices by JAX's collectives and lax.ppermute only.
A program may use at most 64 MiB of HBM per device.

```python
import math
import jax
import jax.numpy as jnp
import numpy as np
from jax import lax

D = 2048
FF = 768
TOK_DEV = 512
EXPERTS = 8
TOKENS = 16384
MOST = 128
CAP = 2048


def block_scale(own_key, dims, pieces, least, high):
    loudness, own = 1.0, jax.random.fold_in(own_key, 6)
    for position, blocks in pieces:
        draws = jnp.exp(jax.random.uniform(jax.random.fold_in(own, position), (blocks,), jnp.float32, least / len(pieces), high / len(pieces)))
        loudness = loudness * jnp.repeat(draws, dims[position] // blocks).reshape([-1 if axis == position else 1 for axis in range(len(dims))])
    return loudness


def routed_block(stream_key, own, number, rows, number_of, top, reach, lean):
    sequence = jax.random.permutation(stream_key, number_of)
    crowded, common = portions_of(number_of, rows * top, reach, lean, True), portions_of(number_of, rows * top, reach, lean, False)
    places = jnp.arange(number_of)

    def named(sizes, turn):
        used = int((sizes > 0).sum())
        fixed = max(1, used // 4)
        shifted = fixed + (places - fixed + turn * (used - fixed)) % max(1, number_of - fixed)
        return jnp.zeros((number_of,), jnp.int32).at[sequence[jnp.where(places < fixed, places, shifted)]].set(jnp.asarray(sizes, jnp.int32))

    sizes = jnp.where(number % 4 == 0, named(crowded, number // 4), named(common, number - number // 4 - 1))
    mixed = jax.random.permutation(jax.random.fold_in(own, 3), number_of)
    donor, taker = mixed[0:number_of // 2 * 2:2], mixed[1:number_of // 2 * 2:2]
    slack = jnp.minimum(sizes[donor] - 1, reach - sizes[taker]) // 2
    slack = jnp.where((donor == sequence[0]) | (taker == sequence[0]) | (sizes[taker] == 0), 0, jnp.maximum(slack, 0))
    shifted = jax.random.randint(jax.random.fold_in(own, 4), (number_of // 2,), 0, 1 << 20) % (slack + 1)
    sizes = sizes.at[donor].add(-shifted).at[taker].add(shifted)
    items = jnp.searchsorted(jnp.cumsum(sizes), jnp.arange(rows * top), side="right").astype(jnp.int32)
    table = items.reshape(top, rows).T
    table = table[jax.random.permutation(jax.random.fold_in(own, 1), rows)]
    turn = jax.random.randint(jax.random.fold_in(own, 2), (rows, 1), 0, top)
    return jnp.take_along_axis(table, (jnp.arange(top)[None, :] + turn) % top, axis=1)


def portions_of(number_of, total, most, slope, full):
    weights = [(1 << 20) // math.isqrt(standing ** slope) + 1 for standing in range(1, number_of + 1)]
    largest = most if full else min(most, max(-(-total // number_of), total * weights[0] // sum(weights)))
    least = 1 if total - largest >= number_of - 1 else 0
    holding, rest = [largest] + [least] * (number_of - 1), total - largest - least * (number_of - 1)
    while rest > 0:
        candidates = [i for i in range(1, number_of) if holding[i] < largest] or [i for i in range(1, number_of) if holding[i] < most]
        pool, left = sum([weights[i] for i in candidates]), rest
        for i in candidates:
            more = min(most - holding[i], max(1, left * weights[i] // pool), rest)
            holding[i] = holding[i] + more
            rest = rest - more
    return np.array(holding)


def scatter_about(key, dims, spread, bound, cuts=(), kind=jnp.bfloat16):
    factor_of = block_scale(key, dims, cuts, -0.22, 0.18) if cuts else 1.0
    result = jax.random.normal(key, dims, jnp.float32) * spread * factor_of
    return jnp.minimum(jnp.maximum(result, -bound), bound).astype(kind)


def setup_inputs(seed: int = 0) -> dict:
    arg_keys = jax.random.split(jax.random.key(seed), 6)
    tokens = scatter_about(arg_keys[0], (TOKENS, D), 1.0, 6.0, ((0, 32),))
    expert_ids_keys = jax.random.split(jax.random.fold_in(arg_keys[1], 1), TOKENS // TOK_DEV)
    expert_ids_turns = jax.random.permutation(jax.random.fold_in(arg_keys[1], 3), TOKENS // TOK_DEV)
    expert_ids = jax.vmap(lambda own, number: routed_block(jax.random.fold_in(arg_keys[1], 2), own, number, TOK_DEV, EXPERTS, 1, MOST, 2))(expert_ids_keys, expert_ids_turns).reshape((TOKENS, 1))
    gate_proj = scatter_about(arg_keys[2], (EXPERTS, D, FF), D ** -0.5, 0.125, ((0, 8),))
    up_proj = scatter_about(arg_keys[3], (EXPERTS, D, FF), D ** -0.5, 0.125, ((0, 8),))
    down_proj = scatter_about(arg_keys[4], (EXPERTS, FF, D), FF ** -0.5, 0.21875, ((0, 8),))
    return {"tokens": tokens, "expert_ids": expert_ids, "gate_proj": gate_proj, "up_proj": up_proj, "down_proj": down_proj}


def expert_ffn(args):
    rows, gate_w, up_w, down_w = args
    gate_val = jnp.dot(rows, gate_w, preferred_element_type=jnp.float32)
    up_val = jnp.dot(rows, up_w, preferred_element_type=jnp.float32)
    hidden = (jax.nn.silu(gate_val) * up_val).astype(jnp.bfloat16)
    return jnp.dot(hidden, down_w, preferred_element_type=jnp.float32).astype(jnp.bfloat16)


def reference(tokens, expert_ids, gate_proj, up_proj, down_proj):
    choices = expert_ids[:, 0].astype(jnp.int32)
    onehot = (choices[:, None] == jnp.arange(EXPERTS, dtype=jnp.int32)[None, :]).astype(jnp.int32)
    before = jnp.cumsum(onehot, axis=0) - onehot
    slot_index = jnp.sum(before * onehot, axis=1).astype(jnp.int32)
    is_kept = slot_index < CAP
    buffer = jnp.zeros((EXPERTS, CAP, D), tokens.dtype)
    buffer = buffer.at[choices, slot_index].set(tokens, mode="drop")
    results = lax.map(expert_ffn, (buffer, gate_proj, up_proj, down_proj))
    picked = results[choices, jnp.minimum(slot_index, CAP - 1)]
    mixed = jnp.where(is_kept[:, None], picked, jnp.zeros_like(picked))
    return mixed, slot_index
```

```python
import functools
import jax
import jax.numpy as jnp
from jax import lax
from jax.experimental import pallas as pl
from jax.experimental.pallas import tpu as pltpu
from jax.sharding import PartitionSpec as P

VMEM = pltpu.VMEM
LATE = 1


def after(value, *done):
    return lax.optimization_barrier((value, done))[0]


def targets_of(spans, axis, shape):
    index = lax.broadcasted_iota(jnp.int32, shape, axis)
    result, first = None, 0
    for start, rows in spans:
        shifted = index + (start - first)
        result = shifted if result is None else jnp.where(index >= first, shifted, result)
        first += rows
    return result


def pack_rows(spans, place, tokens, outs):
    total = sum(rows for _, rows in spans)
    chosen = targets_of(spans, 0, (total, place.shape[1])) == place
    picked = jnp.dot(
        jnp.where(chosen, 1.0, 0.0).astype(jnp.bfloat16), tokens, preferred_element_type=jnp.float32
    ).astype(jnp.bfloat16)
    first = 0
    for (_, rows), out in zip(spans, outs):
        out[...] = picked[first : first + rows, :]
        first += rows


def route_kernel(experts_all, most, spans, me_ref, ids_ref, tokens_ref, rank_ref, place_ref, *outs):
    ids = ids_ref[...]
    count = ids.shape[1]
    onehot = lax.broadcasted_iota(jnp.int32, (experts_all, count), 0) == ids
    earlier = lax.broadcasted_iota(jnp.int32, (count, count), 0) < lax.broadcasted_iota(
        jnp.int32, (count, count), 1
    )
    before = jnp.dot(
        jnp.where(onehot, 1.0, 0.0).astype(jnp.bfloat16),
        jnp.where(earlier, 1.0, 0.0).astype(jnp.bfloat16),
        preferred_element_type=jnp.float32,
    )
    rank = jnp.sum(jnp.where(onehot, before, 0.0), axis=0, keepdims=True).astype(jnp.int32)
    place = (ids ^ me_ref[0]) * most + rank
    rank_ref[...] = rank
    place_ref[...] = place
    pack_rows(spans, place, tokens_ref[...], outs)


def pack_kernel(spans, place_ref, tokens_ref, *outs):
    pack_rows(spans, place_ref[...], tokens_ref[...], outs)


def combine_kernel(spans, has_part, place_ref, *refs):
    blocks, out, held = refs[: len(spans)], refs[-2], refs[-1]
    first = 0
    for (_, rows), block in zip(spans, blocks):
        held[first : first + rows, :] = block[...]
        first += rows
    place = place_ref[...]
    chosen = place == targets_of(spans, 1, (place.shape[0], first))
    total = jnp.dot(
        jnp.where(chosen, 1.0, 0.0).astype(jnp.bfloat16), held[...], preferred_element_type=jnp.float32
    )
    if has_part:
        total = total + refs[len(spans)][...].astype(jnp.float32)
    out[...] = total.astype(out.dtype)


def ffn_kernel(sizes, steps, *refs):
    count = len(sizes)
    blocks = refs[:count]
    gate_ref, up_ref, down_ref = refs[count : count + 3]
    outs = refs[count + 3 : 2 * count + 3]
    held, total = refs[2 * count + 3 :]
    step = pl.program_id(0)

    @pl.when(step == 0)
    def _():
        start = 0
        for size, block in zip(sizes, blocks):
            held[start : start + size, :] = block[...]
            start += size

    rows = held[...]
    gate_val = jnp.dot(rows, gate_ref[...], preferred_element_type=jnp.float32)
    up_val = jnp.dot(rows, up_ref[...], preferred_element_type=jnp.float32)
    hidden = (gate_val / (1.0 + jnp.exp(-gate_val)) * up_val).astype(jnp.bfloat16)
    part = jnp.dot(hidden, down_ref[...], preferred_element_type=jnp.float32)

    @pl.when(step == 0)
    def _():
        total[...] = part

    @pl.when((step > 0) & (step < steps - 1))
    def _():
        total[...] += part

    @pl.when(step == steps - 1)
    def _():
        whole = total[...] + part if steps > 1 else part
        start = 0
        for size, out in zip(sizes, outs):
            out[...] = whole[start : start + size, :].astype(out.dtype)
            start += size


def expert_ffn(blocks, gate_proj, up_proj, down_proj):
    _, width, inner = gate_proj.shape
    chunk = 256 if inner % 256 == 0 else inner
    steps = inner // chunk
    sizes = [block.shape[0] for block in blocks]
    total = sum(sizes)
    rows_specs = [pl.BlockSpec(block.shape, lambda i: (0, 0)) for block in blocks]
    return pl.pallas_call(
        functools.partial(ffn_kernel, sizes, steps),
        grid=(steps,),
        in_specs=rows_specs
        + [
            pl.BlockSpec((None, width, chunk), lambda i: (0, 0, i)),
            pl.BlockSpec((None, width, chunk), lambda i: (0, 0, i)),
            pl.BlockSpec((None, chunk, width), lambda i: (0, i, 0)),
        ],
        out_specs=rows_specs,
        out_shape=[jax.ShapeDtypeStruct(block.shape, jnp.bfloat16) for block in blocks],
        scratch_shapes=[VMEM((total, width), jnp.bfloat16), VMEM((total, width), jnp.float32)],
        cost_estimate=pl.CostEstimate(
            flops=6 * total * width * inner,
            bytes_accessed=6 * width * inner + 4 * total * width,
            transcendentals=total * inner,
        ),
        name="expert_ffn",
    )(*blocks, gate_proj, up_proj, down_proj)


def in_vmem(count):
    return [pl.BlockSpec(memory_space=VMEM) for _ in range(count)]


def shift_small(value, axis, size, offset):
    return lax.ppermute(value, axis, [(i, i ^ offset) for i in range(size)])


def extra_exchange(block, levels_up, levels_down, is_low, step, size, offset):
    up_pairs = [(i, i ^ offset) for i in range(size) if i < i ^ offset]
    down_pairs = [(i ^ offset, i) for i, _ in up_pairs]
    most = block.shape[0]
    levels = most // step

    def branch(up, down):
        def run(value):
            got = []
            for level, pairs in ((up, up_pairs), (down, down_pairs)):
                if level:
                    part = lax.ppermute(value[: level * step], "expert", pairs)
                    got.append(jnp.pad(part, ((0, most - level * step), (0, 0))))
            if not got:
                return jnp.zeros_like(value)
            if len(got) == 2:
                return jnp.where(is_low, got[1], got[0])
            return got[0]

        return run

    branches = [branch(up, down) for up in range(levels + 1) for down in range(levels + 1)]
    return lax.switch(levels_up * (levels + 1) + levels_down, branches, block)


def on_device(tokens, expert_ids, gate_proj, up_proj, down_proj):
    tok_rows, width = tokens.shape
    experts_all = lax.axis_size("expert")
    shards = lax.axis_size("dp")
    most = 2 * tok_rows // experts_all
    capacity = tok_rows * shards
    me = lax.axis_index("expert")
    shard = lax.axis_index("dp")
    ids = expert_ids.reshape(1, tok_rows)
    weights = (gate_proj, up_proj, down_proj)
    split = most >= 64
    base = most // 2 if split else most
    step = (most - base) // 2 if split else 0
    half = experts_all // 2

    experts = jnp.arange(experts_all, dtype=jnp.int32)
    counts = jnp.sum((ids.reshape(tok_rows, 1) == experts[None, :]).astype(jnp.int32), axis=0)
    near = list(range(1, half))
    beside = [k for k in near if k > 1]
    far = list(range(half, experts_all))
    quarter = max(half // 2, 1)
    block = lambda rows: jax.ShapeDtypeStruct((rows, width), jnp.bfloat16)
    counts_of = {0: counts}
    for k in far:
        counts_of[k] = shift_small(counts, "expert", experts_all, k)

    spans_a = [(k * most, most) for k in beside] + [(k * most, base) for k in far]
    rank, place, *sent = pl.pallas_call(
        functools.partial(route_kernel, experts_all, most, spans_a),
        in_specs=[pl.BlockSpec(memory_space=pltpu.SMEM)] + in_vmem(2),
        out_specs=in_vmem(2 + len(spans_a)),
        out_shape=[jax.ShapeDtypeStruct((1, tok_rows), jnp.int32)] * 2
        + [block(rows) for _, rows in spans_a],
        name="route",
    )(me.reshape(1), ids, tokens)
    sent = dict(zip(beside + far, sent))
    rest = [0] + near[:1]
    spans_b = [(k * most, most) for k in rest]
    spans_b += [(k * most + base, most - base) for k in far] if split else []
    packed = pl.pallas_call(
        functools.partial(pack_kernel, spans_b),
        in_specs=in_vmem(2),
        out_specs=in_vmem(len(spans_b)),
        out_shape=[block(rows) for _, rows in spans_b],
        name="pack",
    )(place, tokens)
    own = packed[0]
    sent.update(zip(near[:1], packed[1:]))
    extra = dict(zip(far, packed[len(rest) :]))

    arrived = {0: own}
    held_back = far[len(far) - LATE :] if split else []
    for k in beside + [k for k in far if k not in held_back]:
        arrived[k] = shift_small(sent[k], "expert", experts_all, k)
    for k in near[:1]:
        arrived[k] = shift_small(sent[k], "expert", experts_all, k)
    for k in near:
        counts_of[k] = shift_small(after(counts, own), "expert", experts_all, k)

    def send_extra(k, value, returning):
        mine, theirs = counts[me ^ k], counts_of[k][me]
        level = lambda n: jnp.clip((n - base + step - 1) // step, 0, (most - base) // step)
        is_low = me < (me ^ k)
        out_level, in_level = level(mine), level(theirs)
        if returning:
            out_level, in_level = in_level, out_level
        up = jnp.where(is_low, out_level, in_level)
        down = jnp.where(is_low, in_level, out_level)
        return extra_exchange(value, up, down, is_low, step, experts_all, k)

    done = {}
    last = own
    group = [0] + near
    for first in range(0, len(group), quarter):
        part = group[first : first + quarter]
        results = expert_ffn([after(arrived[part[0]], last)] + [arrived[k] for k in part[1:]], *weights)
        last = results[0]
        done.update(zip(part, results))
    back, back_extra, returns = {0: done[0]}, {}, {}
    for first in range(0, len(far), quarter):
        part = far[first : first + quarter]
        extras = []
        if split:
            for k in part:
                last = send_extra(k, after(extra[k], last), False)
                extras.append(last)
            if first == 0:
                for k in held_back:
                    arrived[k] = shift_small(after(sent[k], last), "expert", experts_all, k)
        results = expert_ffn([arrived[k] for k in part] + extras, *weights)
        last = results[0]
        for i, k in enumerate(part):
            back[k] = shift_small(results[i], "expert", experts_all, k)
            if split:
                returns[k] = results[len(part) + i]
    for k in near:
        back[k] = shift_small(after(done[k], last), "expert", experts_all, k)

    every = jnp.stack([counts_of[k] for k in range(experts_all)])
    inner = jnp.sum(jnp.where(((me ^ experts) < me)[:, None], every, 0), axis=0)
    shard_totals = lax.all_gather(after(jnp.sum(every, axis=0), last), "dp")
    earlier = jnp.arange(shards, dtype=jnp.int32) < shard
    outer = jnp.sum(jnp.where(earlier[:, None], shard_totals, 0), axis=0)
    onehot = (ids == experts[:, None]).astype(jnp.int32)
    slot = jnp.sum(onehot * (inner + outer)[:, None], axis=0, keepdims=True) + rank
    kept_place = jnp.where(slot < capacity, place, -1).reshape(tok_rows, 1)

    def combine(keys, extra_keys, part):
        spans = [(k * most, back[k].shape[0]) for k in keys]
        spans += [(k * most + base, most - base) for k in extra_keys]
        operands = [back[k] for k in keys] + [back_extra[k] for k in extra_keys]
        if part is not None:
            operands.append(part)
        return pl.pallas_call(
            functools.partial(combine_kernel, spans, part is not None),
            in_specs=in_vmem(1 + len(operands)),
            out_specs=pl.BlockSpec(memory_space=VMEM),
            out_shape=block(tok_rows),
            scratch_shapes=[VMEM((sum(rows for _, rows in spans), width), jnp.bfloat16)],
            name="combine",
        )(kept_place, *operands)

    mixed = combine(rest + far[:quarter], [], None)
    last = mixed
    if split:
        for k in far[:-1]:
            last = send_extra(k, after(returns[k], last), True)
            back_extra[k] = last
    mixed = combine(beside + far[quarter:], [], after(mixed, last))
    if split:
        back_extra[far[-1]] = send_extra(far[-1], after(returns[far[-1]], mixed), True)
        back_keys = list(far)
        mixed = combine([], back_keys, mixed)
    return (mixed, slot.reshape(tok_rows))


def solution(mesh):
    in_specs = (
        P(("dp", "expert"), None),
        P(("dp", "expert"), None),
        P("expert", None, None),
        P("expert", None, None),
        P("expert", None, None),
    )
    out_specs = (P(("dp", "expert"), None), P(("dp", "expert")))
    return jax.shard_map(
        on_device, mesh=mesh, in_specs=in_specs, out_specs=out_specs, check_vma=False
    )
```

```python
import functools
import jax
import jax.numpy as jnp
from jax import lax
from jax.experimental import pallas as pl
from jax.experimental.pallas import tpu as pltpu
from jax.sharding import PartitionSpec as P


VMEM = pltpu.VMEM
BF16 = jnp.bfloat16
LIMIT = pltpu.CompilerParams(vmem_limit_bytes=20 * 2**20)


def after(value, *done):
    return lax.optimization_barrier((value, done))[0]


def near_core(value):
    return pltpu.with_memory_space_constraint(value, VMEM)


def in_hbm(value):
    return pltpu.with_memory_space_constraint(value, pltpu.HBM)


def targets_of(spans, axis, shape):
    index = lax.broadcasted_iota(jnp.int32, shape, axis)
    result, first = jnp.full(shape, -7, jnp.int32), 0
    for start, used, rows in spans:
        inside = (index >= first) & (index < first + used)
        result = jnp.where(inside, index + (start - first), result)
        first += rows
    return result


def pack_rows(spans, place, tokens, outs):
    total = sum(rows for _, _, rows in spans)
    chosen = targets_of(spans, 0, (total, place.shape[1])) == place
    picked = jnp.dot(
        jnp.where(chosen, 1.0, 0.0).astype(BF16), tokens, preferred_element_type=jnp.float32
    ).astype(BF16)
    first = 0
    for (_, _, rows), out in zip(spans, outs):
        out[...] = picked[first : first + rows, :]
        first += rows


def route_kernel(experts_all, most, spans, me_ref, ids_ref, tokens_ref, *refs):
    rank_ref, place_ref, counts_ref = refs[:3]
    ids = ids_ref[...]
    count = ids.shape[1]
    onehot = lax.broadcasted_iota(jnp.int32, (experts_all, count), 0) == ids
    earlier = lax.broadcasted_iota(jnp.int32, (count, count), 0) < lax.broadcasted_iota(
        jnp.int32, (count, count), 1
    )
    before = jnp.dot(
        jnp.where(onehot, 1.0, 0.0).astype(BF16),
        jnp.where(earlier, 1.0, 0.0).astype(BF16),
        preferred_element_type=jnp.float32,
    )
    rank = jnp.sum(jnp.where(onehot, before, 0.0), axis=0, keepdims=True).astype(jnp.int32)
    place = (ids ^ me_ref[0]) * most + rank
    rank_ref[...] = rank
    place_ref[...] = place
    counts = jnp.sum(jnp.where(onehot, 1.0, 0.0), axis=1, keepdims=True)
    shape = (experts_all, 128)
    diagonal = lax.broadcasted_iota(jnp.int32, shape, 0) == lax.broadcasted_iota(jnp.int32, shape, 1)
    counts_ref[...] = jnp.sum(jnp.where(diagonal, counts, 0.0), axis=0, keepdims=True).astype(jnp.int32)
    pack_rows(spans, place, tokens_ref[...], refs[3:])


def pack_kernel(spans, place_ref, tokens_ref, *outs):
    pack_rows(spans, place_ref[...], tokens_ref[...], outs)


def combine_kernel(spans, has_part, place_ref, *refs):
    count = len(spans)
    blocks, out, held = refs[:count], refs[-2], refs[-1]

    @pl.when(pl.program_id(0) == 0)
    def _():
        first = 0
        for (_, _, rows), block in zip(spans, blocks):
            held[first : first + rows, :] = block[...]
            first += rows

    place = place_ref[...]
    chosen = place == targets_of(spans, 1, (place.shape[0], held.shape[0]))
    total = jnp.dot(
        jnp.where(chosen, 1.0, 0.0).astype(BF16), held[...], preferred_element_type=jnp.float32
    )
    if has_part:
        total = total + refs[count][...].astype(jnp.float32)
    out[...] = total.astype(out.dtype)


def ffn_kernel(sizes, steps, *refs):
    count = len(sizes)
    blocks = refs[:count]
    gate_ref, up_ref, down_ref = refs[count : count + 3]
    outs = refs[count + 3 : 2 * count + 3]
    held, total = refs[2 * count + 3 :]
    step = pl.program_id(0)

    @pl.when(step == 0)
    def _():
        first = 0
        for size, block in zip(sizes, blocks):
            held[first : first + size, :] = block[...]
            first += size

    rows = held[...]
    gate_val = jnp.dot(rows, gate_ref[...], preferred_element_type=jnp.float32)
    up_val = jnp.dot(rows, up_ref[...], preferred_element_type=jnp.float32)
    hidden = (gate_val / (1.0 + jnp.exp(-gate_val)) * up_val).astype(BF16)
    part = jnp.dot(hidden, down_ref[...], preferred_element_type=jnp.float32)

    @pl.when(step == 0)
    def _():
        total[...] = part

    @pl.when((step > 0) & (step < steps - 1))
    def _():
        total[...] += part

    @pl.when(step == steps - 1)
    def _():
        whole = total[...] + part if steps > 1 else part
        first = 0
        for size, out in zip(sizes, outs):
            out[...] = whole[first : first + size, :].astype(out.dtype)
            first += size


def in_vmem(count):
    return [pl.BlockSpec(memory_space=VMEM) for _ in range(count)]


def expert_ffn(arrived, others, weights):
    _, width, inner = weights[0].shape
    chunk = 256 if inner % 256 == 0 else inner
    steps = inner // chunk
    blocks = arrived + others
    sizes = [block.shape[0] for block in blocks]
    rows_specs = [pl.BlockSpec(block.shape, lambda i: (0, 0)) for block in blocks]
    scratch = (sum(sizes), width)
    return pl.pallas_call(
        functools.partial(ffn_kernel, sizes, steps),
        grid=(steps,),
        in_specs=in_vmem(len(arrived))
        + rows_specs[len(arrived) :]
        + [
            pl.BlockSpec((None, width, chunk), lambda i: (0, 0, i)),
            pl.BlockSpec((None, width, chunk), lambda i: (0, 0, i)),
            pl.BlockSpec((None, chunk, width), lambda i: (0, i, 0)),
        ],
        out_specs=rows_specs,
        out_shape=[pltpu.HBM(block.shape, BF16) for block in blocks],
        scratch_shapes=[VMEM(scratch, BF16), VMEM(scratch, jnp.float32)],
        compiler_params=LIMIT,
        name="expert_ffn",
    )(*[near_core(block) for block in arrived], *[in_hbm(value) for value in others], *[in_hbm(value) for value in weights])


def shift(value, size, offset):
    return lax.ppermute(value, "expert", [(i, i ^ offset) for i in range(size)])


def extra_exchange(block, up, down, size, offset):
    pairs = [(i, i ^ offset) for i in range(size)]
    rising = [pair for pair in pairs if pair[0] < pair[1]]
    falling = [pair for pair in pairs if pair[0] > pair[1]]
    branches = [lambda value: value] + [
        lambda value, chosen=chosen: lax.ppermute(value, "expert", chosen)
        for chosen in (falling, rising, pairs)
    ]
    return lax.switch(2 * up + down, branches, block)


def on_device(tokens, expert_ids, gate_proj, up_proj, down_proj):
    tok_rows, width = tokens.shape
    experts_all = lax.axis_size("expert")
    shards = lax.axis_size("dp")
    most = 2 * tok_rows // experts_all
    capacity = tok_rows * shards
    me = lax.axis_index("expert")
    shard = lax.axis_index("dp")
    ids = expert_ids.reshape(1, tok_rows)
    weights = (gate_proj, up_proj, down_proj)
    half = experts_all // 2
    split = most >= 64
    base = 5 * most // 8 if split else most

    experts = jnp.arange(experts_all, dtype=jnp.int32)
    near = list(range(1, half))
    beside = [k for k in near if k > 1]
    far = list(range(half, experts_all))
    quarter = max(half // 2, 1)
    block = lambda rows: pltpu.HBM((rows, width), BF16)
    whole_span = lambda k: (k * most, most, most)
    base_span = lambda k: (k * most, base, base)
    extra_span = lambda k: (k * most + base, most - base, most - base)

    def send(value, k):
        return shift(value, experts_all, k)

    spans_a = [whole_span(k) for k in beside] + [base_span(k) for k in far]
    rank, place, counts, *sent = pl.pallas_call(
        functools.partial(route_kernel, experts_all, most, spans_a),
        in_specs=[pl.BlockSpec(memory_space=pltpu.SMEM)] + in_vmem(2),
        out_specs=in_vmem(3 + len(spans_a)),
        out_shape=[jax.ShapeDtypeStruct((1, tok_rows), jnp.int32)] * 2
        + [jax.ShapeDtypeStruct((1, 128), jnp.int32)]
        + [block(rows) for _, _, rows in spans_a],
        compiler_params=LIMIT,
        name="route",
    )(me.reshape(1), ids, in_hbm(tokens))
    counts = counts[0, :experts_all]
    sent = dict(zip(beside + far, sent))
    rest = [0] + near[:1]
    spans_b = [whole_span(k) for k in rest] + ([extra_span(k) for k in far] if split else [])
    packed = pl.pallas_call(
        functools.partial(pack_kernel, spans_b),
        in_specs=in_vmem(2),
        out_specs=in_vmem(len(spans_b)),
        out_shape=[block(rows) for _, _, rows in spans_b],
        compiler_params=LIMIT,
        name="pack",
    )(place, in_hbm(tokens))
    own = packed[0]
    sent.update(zip(near[:1], packed[1:]))
    extra = dict(zip(far, packed[len(rest) :]))

    late = far[quarter + 1 :] if split else []
    arrived, counts_of = {0: own}, {0: counts}
    for k in beside + far + near[:1]:
        if k not in late:
            arrived[k] = send(sent[k], k)
    for k in far + near:
        counts_of[k] = send(counts, k)

    is_low = me < half
    codes = {}

    def send_extra(k, value, returning):
        if k not in codes:
            need = lambda n: (n > base).astype(jnp.int32)
            codes[k] = need(counts[me ^ k]), need(counts_of[k][me])
        out_need, in_need = codes[k][::-1] if returning else codes[k]
        up = jnp.where(is_low, out_need, in_need)
        down = jnp.where(is_low, in_need, out_need)
        return extra_exchange(value, up, down, experts_all, k)

    done, back, back_extra = {}, {}, {}
    last = own
    extras = {}
    if split:
        for k in far[:quarter]:
            last = extras[k] = send_extra(k, after(extra[k], last), False)
        for k in late:
            arrived[k] = send(after(sent[k], last), k)
    returns = {}

    def far_ffn(part):
        results = expert_ffn(
            [arrived[k] for k in part], [extras[k] for k in part] if split else [], weights
        )
        done.update(zip(part, results))
        returns.update(zip(part, results[len(part) :]))
        return results[0]

    last = far_ffn(far[:quarter])
    if split:
        for k in far[quarter:]:
            last = extras[k] = send_extra(k, after(extra[k], last), False)
    for k in far[:quarter]:
        back[k] = send(after(done[k], last), k)
    last = far_ffn(far[quarter:])
    for k in far[quarter:]:
        back[k] = send(done[k], k)
    group = [0] + near
    step = 4 if split else quarter
    for first in range(0, len(group), step):
        part = group[first : first + step]
        results = expert_ffn(
            [after(arrived[k], last) for k in part if k], [arrived[k] for k in part if not k], weights
        )
        done.update(zip([k for k in part if k] + [k for k in part if not k], results))
    back[0] = done[0]
    for k in near:
        back[k] = send(done[k], k)


    every = jnp.stack([counts_of[k] for k in range(experts_all)])
    inner = jnp.sum(jnp.where(((me ^ experts) < me)[:, None], every, 0), axis=0)
    shard_totals = lax.all_gather(after(jnp.sum(every, axis=0), last), "dp")
    earlier = jnp.arange(shards, dtype=jnp.int32) < shard
    outer = jnp.sum(jnp.where(earlier[:, None], shard_totals, 0), axis=0)
    onehot = (ids == experts[:, None]).astype(jnp.int32)
    slot = jnp.sum(onehot * (inner + outer)[:, None], axis=0, keepdims=True) + rank
    kept_place = jnp.where(slot < capacity, place, -1).reshape(tok_rows, 1)

    def combine(keys, extra_keys, part):
        spans = [whole_span(k) if back[k].shape[0] == most else base_span(k) for k in keys]
        spans += [extra_span(k) for k in extra_keys]
        inside = [k for k in keys if k]
        spans = [spans[keys.index(k)] for k in inside] + [
            span for k, span in zip(keys, spans) if not k
        ] + spans[len(keys) :]
        operands = [near_core(back[k]) for k in inside]
        moved = [in_hbm(back[k]) for k in keys if not k] + [in_hbm(back_extra[k]) for k in extra_keys]
        tile = min(tok_rows, 128)
        by_tile = lambda shape: pl.BlockSpec((tile,) + shape[1:], lambda i: (i, 0))
        whole = lambda value: pl.BlockSpec(value.shape, lambda i: (0, 0))
        specs = [by_tile(kept_place.shape)] + in_vmem(len(operands)) + [whole(v) for v in moved]
        operands += moved
        if part is not None:
            operands.append(in_hbm(part))
            specs.append(by_tile(part.shape))
        return pl.pallas_call(
            functools.partial(combine_kernel, spans, part is not None),
            grid=(tok_rows // tile,),
            in_specs=specs,
            out_specs=by_tile((tok_rows, width)),
            out_shape=block(tok_rows),
            scratch_shapes=[VMEM((sum(rows for _, _, rows in spans), width), BF16)],
            compiler_params=LIMIT,
            name="combine",
        )(kept_place, *operands)

    last = mixed = combine([0] + far[:quarter], [], None)
    if split:
        for k in far[:-1]:
            last = back_extra[k] = send_extra(k, after(returns[k], last), True)
    mixed = combine(near + far[quarter:], [], after(mixed, last))
    if split:
        back_extra[far[-1]] = send_extra(far[-1], after(returns[far[-1]], mixed), True)
        mixed = combine([], far, mixed)
    return (mixed, slot.reshape(tok_rows))


def solution(mesh):
    in_specs = (
        P(("dp", "expert"), None),
        P(("dp", "expert"), None),
        P("expert", None, None),
        P("expert", None, None),
        P("expert", None, None),
    )
    out_specs = (P(("dp", "expert"), None), P(("dp", "expert")))

    return jax.shard_map(
        on_device, mesh=mesh, in_specs=in_specs, out_specs=out_specs, check_vma=False
    )
```
